128 devices in a mesh: tp: 16 (over z, y), dp: 8 (over x, core).
Axes of the slice: x: 4, y: 4, z: 4, core: 2. Of those that a mesh axis runs over, the one named last changes fastest.
Arguments:
- hidden: bfloat16 [4096, 1536], P('dp')
- labels: int32 [4096], P('dp')
- loss_mask: int32 [4096], P('dp')
- norm_gain: bfloat16 [1536], replicated
- w_out: bfloat16 [1536, 151936], P(None, 'tp')
Outputs:
- output 1: float32 [], replicated
- output 2: bfloat16 [4096, 1536], P('dp')
- output 3: float32 [1536, 151936], P(None, 'tp')
- output 4: float32 [1536], replicated
All inputs are finite; a program needn't handle non-finite values.
Results may differ from the reference program's by a relative error of at most 0.001.
Values sent between devices are 32-bit elements.
A program may use at most 1 GiB of HBM per device.

```python
import math
import jax
import jax.numpy as jnp
from jax import lax

D = 1536
V = 151936
TOKENS_DEV = 512
DATA_SHARDS = 8
TOKENS = TOKENS_DEV * DATA_SHARDS
NORM_EPS = 1e-5


def setup_inputs(seed: int = 0) -> dict:
    rng_key = jax.random.key(seed)
    k_hid, k_lab, k_dens, k_draw, k_gain, k_wout = jax.random.split(rng_key, 6)
    hidden = jax.random.normal(k_hid, (TOKENS, D), jnp.float32)
    labels = jax.random.randint(k_lab, (TOKENS,), 0, V, dtype=jnp.int32)
    labels = labels.at[0].set(V - 1).at[1].set(0)
    density = jax.random.randint(k_dens, (DATA_SHARDS, 1), 20, 96, dtype=jnp.int32)
    coin_draws = jax.random.randint(k_draw, (DATA_SHARDS, TOKENS_DEV), 0, 100, dtype=jnp.int32)
    loss_mask = (coin_draws < density).astype(jnp.int32).reshape(TOKENS).at[0].set(1)
    norm_gain = 1.0 + 0.3 * jax.random.normal(k_gain, (D,), jnp.float32)
    w_scale = math.sqrt(math.log(V) / D)
    w_out = w_scale * jax.random.normal(k_wout, (D, V), jnp.float32)
    return {"hidden": hidden.astype(jnp.bfloat16), "labels": labels, "loss_mask": loss_mask, "norm_gain": norm_gain.astype(jnp.bfloat16), "w_out": w_out.astype(jnp.bfloat16)}


def reference(hidden, labels, loss_mask, norm_gain, w_out):
    mask_f = loss_mask.astype(jnp.float32)
    mask_total = jnp.sum(mask_f)
    gain_f = norm_gain.astype(jnp.float32)
    vocab_ids = jnp.arange(V, dtype=jnp.int32)

    def block_step(acc_in, row_block):
        loss_acc, dw_acc, dgain_acc = acc_in
        h_block, lab_block, mask_block = row_block
        h_f32 = h_block.astype(jnp.float32)
        r_inv = lax.rsqrt(jnp.mean(h_f32 * h_f32, axis=-1, keepdims=True) + NORM_EPS)
        x_hat = h_f32 * r_inv
        normed = (x_hat * gain_f).astype(jnp.bfloat16)
        logits = jnp.dot(normed, w_out, preferred_element_type=jnp.float32)
        row_max = jnp.max(logits, axis=-1, keepdims=True)
        log_norm = row_max + jnp.log(jnp.sum(jnp.exp(logits - row_max), axis=-1, keepdims=True))
        target = jnp.take_along_axis(logits, lab_block[:, None], axis=1)
        row_weight = mask_block[:, None] / mask_total
        loss_acc = loss_acc + jnp.sum(row_weight * (log_norm - target))
        onehot = (vocab_ids[None, :] == lab_block[:, None]).astype(jnp.float32)
        d_logits = (row_weight * (jnp.exp(logits - log_norm) - onehot)).astype(jnp.bfloat16)
        d_normed = jnp.dot(d_logits, w_out.T, preferred_element_type=jnp.float32)
        dw_acc = dw_acc + jnp.dot(normed.T, d_logits, preferred_element_type=jnp.float32)
        dgain_acc = dgain_acc + jnp.sum(d_normed * x_hat, axis=0)
        d_xhat = d_normed * gain_f
        d_hid = r_inv * (d_xhat - x_hat * jnp.mean(d_xhat * x_hat, axis=-1, keepdims=True))
        return (loss_acc, dw_acc, dgain_acc), d_hid.astype(jnp.bfloat16)

    row_blocks = (hidden.reshape(DATA_SHARDS, TOKENS_DEV, D), labels.reshape(DATA_SHARDS, TOKENS_DEV), mask_f.reshape(DATA_SHARDS, TOKENS_DEV))
    acc_start = (jnp.zeros((), jnp.float32), jnp.zeros((D, V), jnp.float32), jnp.zeros((D,), jnp.float32))
    (loss_total, d_w_out, d_gain), d_hidden = lax.scan(block_step, acc_start, row_blocks)
    return loss_total, d_hidden.reshape(TOKENS, D), d_w_out, d_gain
```

```python
import functools
import math

import jax
import jax.numpy as jnp
from jax import lax
from jax.experimental import pallas as pl
from jax.experimental.pallas import tpu as pltpu
from jax.sharding import PartitionSpec as P

NORM_EPS = 1e-5
MESH = pl.DeviceIdType.MESH
D = 1536
V_LOC = 9496
ROWS = 4096
CHIP_ROWS = 1024
OWN = 512
TN = 256
TILES = 19
NEG = -3.4028234e38
CHUNKS = (4, 8, 7)
VMEM_LIMIT = 66_000_000


HALVES = (0, 1)
STEPS = (1, 2, 3)
LANES = 128


def cost(macs, nbytes):
    return pl.CostEstimate(flops=2 * macs, bytes_accessed=nbytes, transcendentals=0)


def row_block(shape, f):
    return pl.BlockSpec(shape, lambda t, s: (f(t, s), 0))


def axes():
    tp = lax.axis_index("tp")
    dp = lax.axis_index("dp")
    return lax.div(dp, 2), lax.rem(dp, 2), lax.div(tp, 4), lax.rem(tp, 4)


def dev(x, c, z, y):
    return {"tp": z * 4 + y, "dp": x * 2 + c}


def up(a, n=1):
    return lax.rem(a + n, 4)


CY = 896
COMM_X, COMM_YZ, COMM_XO = 0, 4, 20


def gather_kernel(yf, lm, out, out_lm, ssem, rsem, dssem, drsem, lsem):
    x, c, z, y = axes()
    xp, x2, xm = (up(x, n) for n in STEPS)
    yp, y2, ym = (up(y, n) for n in STEPS)
    zp, z2, zm = (up(z, n) for n in STEPS)
    d_xp, d_xm, d_x2 = (dev(v, c, z, y) for v in (xp, xm, x2))
    d_yp, d_ym = (dev(x, c, z, v) for v in (yp, ym))
    d_zp, d_zm = (dev(x, c, v, y) for v in (zp, zm))
    d_sib = dev(x, 1 - c, z, y)
    others = (xp, x2, xm)
    every = slice(None)
    low, high = pl.ds(0, CY), pl.ds(CY, D - CY)
    log = {}

    barrier = pltpu.get_barrier_semaphore()
    peers = (d_xp, d_xm, d_x2, d_yp, d_ym, d_zp, d_zm, d_sib)
    for d in peers:
        pl.semaphore_signal(barrier, inc=1, device_id=d, device_id_type=MESH)
    pl.semaphore_wait(barrier, len(peers))

    def remote(src, dst, s, r, d):
        return pltpu.make_async_remote_copy(src_ref=src, dst_ref=dst, send_sem=s, recv_sem=r, device_id=d, device_id_type=MESH)

    def view(ref, idx, cols):
        return ref.at[idx + (every,) * (ref.ndim - 1 - len(idx)) + (cols,)]

    def rows_of(idx):
        n = 1
        for size, i in zip(out.shape[:-1], idx + (every,) * out.ndim):
            if isinstance(i, slice):
                n *= size
        return n

    def fwd(idx, k, d, cols=low):
        remote(view(out, idx, cols), view(out, idx, cols), ssem.at[k], rsem.at[k], d).start()
        log[k] = (log.get(k, (0,))[0] + rows_of(idx), cols)

    def sib(idx, k, cols=low):
        remote(view(out, idx, cols), view(out, idx, cols), dssem.at[k], drsem.at[k], d_sib).start()
        log["s", k] = (log.get(("s", k), (0,))[0] + rows_of(idx), cols)

    def waiter(rows, cols, s, r):
        for idx in WAIT_VIEWS:
            ref = view(out, idx, cols)
            if math.prod(ref.shape[:-1]) == rows:
                return remote(ref, ref, s, r, d_sib)
        raise ValueError(rows)

    def got(ks):
        for k in ks:
            waiter(*log[k], ssem.at[k], rsem.at[k]).wait_recv()

    def first(src, idx, k, d, cols):
        remote(view(yf, src, cols), view(out, idx, cols), ssem.at[k], rsem.at[k], d).start()
        log[k] = (rows_of(idx), cols)

    for k, d in enumerate((d_xp, d_xm)):
        first((z, y), (x, c, z, y), COMM_X + k, d, low)
    lm_copies = [remote(lm, out_lm.at[x, c], dssem.at[k], drsem.at[k], d) for k, d in enumerate((d_xp, d_xm, d_x2))]
    own = pltpu.make_async_copy(yf, out.at[x, c], lsem.at[0])
    own_lm = pltpu.make_async_copy(lm, out_lm.at[x, c], lsem.at[1])
    own_sib = remote(yf, out.at[x, c], dssem.at[4], drsem.at[4], d_sib)
    for cp in (*lm_copies, own, own_lm, own_sib):
        cp.start()
    got((COMM_X, COMM_X + 1))
    fwd((xm, c, z, y, 0), COMM_X + 2, d_xp)
    fwd((xp, c, z, y, 1), COMM_X + 3, d_xm)
    for xb in (xm, xp):
        sib((xb, c, z, y), 5)
    got((COMM_X + 2, COMM_X + 3))
    for k, d in enumerate((d_xp, d_xm)):
        first((), (x, c), COMM_XO + k, d, high)
    sib((x2, c, z, y), 6)

    k = COMM_YZ
    for step in HALVES:
        a_own, b_own = ((z, y, 0), (z, y, 1)) if step == 0 else ((z, every, 0), (every, y, 1))
        a_from = (lambda v: (z, v, 0)) if step == 0 else (lambda v: (v, every, 0))
        b_from = (lambda v: (v, y, 1)) if step == 0 else (lambda v: (every, v, 1))
        a_dim = (yp, y2, ym, d_yp, d_ym)
        b_dim = (zp, z2, zm, d_zp, d_zm)
        if step:
            a_dim, b_dim = b_dim, a_dim
        for xb in others:
            for i, (piece, dim) in enumerate(((a_own, a_dim), (b_own, b_dim))):
                fwd((xb, c, *piece), k + 2 * i, dim[3])
                fwd((xb, c, *piece), k + 2 * i + 1, dim[4])
        if step:
            got((COMM_XO, COMM_XO + 1))
            fwd((xm, c, pl.ds(0, 2)), COMM_XO + 2, d_xp, high)
            fwd((xp, c, pl.ds(2, 2)), COMM_XO + 3, d_xm, high)
            log[COMM_XO + 2] = log[COMM_XO + 3] = (OWN // 2, high)
            for xb in (xm, xp):
                sib((xb, c), 11, high)
        got(range(k, k + 4))
        k += 4
        for xb in others:
            for i, (piece, dim) in enumerate(((a_from, a_dim), (b_from, b_dim))):
                fwd((xb, c, *piece(dim[2]), 0), k + 2 * i, dim[3])
                fwd((xb, c, *piece(dim[0]), 1), k + 2 * i + 1, dim[4])
        for xb in others:
            for piece, dim in ((a_from, a_dim), (b_from, b_dim)):
                for v in (dim[0], dim[2]):
                    sib((xb, c, *piece(v)), 7 + 2 * step)
        got(range(k, k + 4))
        k += 4
        for xb in others:
            for piece, dim in ((a_from, a_dim), (b_from, b_dim)):
                sib((xb, c, *piece(dim[1])), 8 + 2 * step)
    got((COMM_XO + 2, COMM_XO + 3))
    sib((x2, c), 12, high)

    for cp in (*lm_copies, own, own_lm):
        cp.wait()
    half = remote(out_lm.at[:, c], out_lm.at[:, c], dssem.at[3], drsem.at[3], d_sib)
    half.start()
    for key, (rows, cols) in log.items():
        if isinstance(key, tuple):
            waiter(rows, cols, dssem.at[key[1]], drsem.at[key[1]]).wait()
        else:
            waiter(rows, cols, ssem.at[key], rsem.at[key]).wait_send()
    own_sib.wait()
    half.wait()


def wait_views():
    part = [pl.ds(0, n) for n in range(1, 4)] + [slice(None)]
    return [(a, b, e, f, g, h) for a in part for b in part[:2] for e in part for f in part for g in part[:2] for h in part[:2]]


WAIT_VIEWS = wait_views()


def gather(yf, lm):
    any_spec = pl.BlockSpec(memory_space=pl.ANY)
    vm = pl.BlockSpec(memory_space=pltpu.VMEM)
    sems = [pltpu.SemaphoreType.DMA((n,)) for n in (24, 24, 13, 13, 2)]
    block = (4, 4, 2, 2, 8, D)
    out, out_lm = pl.pallas_call(
        gather_kernel,
        out_shape=(jax.ShapeDtypeStruct((4, 2, *block), jnp.float32), jax.ShapeDtypeStruct((4, 2, *lm.shape), jnp.int32)),
        in_specs=[vm, vm],
        out_specs=(any_spec, any_spec),
        scratch_shapes=sems,
        compiler_params=pltpu.CompilerParams(collective_id=0, has_side_effects=True),
        name="gather_rows",
    )(yf.reshape(block), lm)
    return out.reshape(ROWS, D), out_lm


RC = 256
LC = 512


def logits_kernel(ids, y_hbm, w_ref, z_ref, ybf_out, st_ref, ybf, m_ref, s_ref, fbuf, sems):
    j = pl.program_id(0)

    def y_copy():
        return pltpu.make_async_copy(ybf, ybf_out, sems.at[2])

    @pl.when(j == 1)
    def _():
        y_copy().start()

    lane = lax.broadcasted_iota(jnp.int32, (1, TN), 1)
    valid = lane < (V_LOC - (ids[0] * TILES + j) * TN)
    w = w_ref[...]

    def dot(i):
        rows = pl.ds(i * RC, RC)
        z = lax.dot_general(ybf[rows, :], w, (((1,), (1,)), ((), ())), preferred_element_type=jnp.float32)
        z_ref[rows, :] = jnp.where(valid, z, -jnp.inf)

    def stat(i):
        rows = pl.ds(i * RC, RC)
        z0, z1 = z_ref[rows, :LANES], z_ref[rows, LANES:]
        m_old = m_ref[rows, :]
        m_new = jnp.maximum(m_old, jnp.maximum(z0, z1))
        s_ref[rows, :] = s_ref[rows, :] * jnp.exp(m_old - m_new) + (jnp.exp(z0 - m_new) + jnp.exp(z1 - m_new))
        m_ref[rows, :] = m_new

    n = ROWS // RC

    def fetch(i):
        return pltpu.make_async_copy(y_hbm.at[pl.ds(i * LC, LC)], fbuf.at[i % 2], sems.at[i % 2])

    def tile_work(opening):
        if opening:
            fetch(0).start()
            fetch(1).start()
            m_ref[...] = jnp.full_like(m_ref, NEG)
            s_ref[...] = jnp.zeros_like(s_ref)
        for i in range(n + 1):
            if opening and i < n and i * RC % LC == 0:
                b = i * RC // LC
                fetch(b).wait()
                ybf[pl.ds(b * LC, LC), :] = fbuf[b % 2].astype(jnp.bfloat16)
                if (b + 2) * LC <= ROWS - LC:
                    fetch(b + 2).start()
            if i < n:
                dot(i)
            if i:
                stat(i - 1)

    pl.when(j == 0)(lambda: tile_work(True))
    pl.when(j > 0)(lambda: tile_work(False))

    @pl.when(j == TILES - 1)
    def _():
        def fin(i, _):
            rows = pl.ds(pl.multiple_of(i * LANES, LANES), LANES)
            mt = m_ref[rows, :].T
            stt = s_ref[rows, :].T
            mm = jnp.max(mt, axis=0, keepdims=True)
            st_ref[0, pl.ds(i, 1), :] = mm
            st_ref[1, pl.ds(i, 1), :] = jnp.sum(stt * jnp.exp(mt - mm), axis=0, keepdims=True)
            return 0
        lax.fori_loop(0, 32, fin, 0, unroll=4)
        y_copy().wait()


def logits(ids, y_all, w_t):
    return pl.pallas_call(
        logits_kernel,
        grid_spec=pltpu.PrefetchScalarGridSpec(
            num_scalar_prefetch=1,
            grid=(TILES,),
            in_specs=[pl.BlockSpec(memory_space=pl.ANY), row_block((TN, D), lambda j, c: c[0] * TILES + j)],
            out_specs=(
                row_block((ROWS, TN), lambda j, c: j),
                pl.BlockSpec(memory_space=pl.ANY),
                pl.BlockSpec((2, 32, LANES), lambda j, c: (0, 0, 0)),
            ),
            scratch_shapes=[
                pltpu.VMEM((ROWS, D), jnp.bfloat16),
                pltpu.VMEM((ROWS, LANES), jnp.float32),
                pltpu.VMEM((ROWS, LANES), jnp.float32),
                pltpu.VMEM((2, LC, D), jnp.float32),
                pltpu.SemaphoreType.DMA((3,)),
            ],
        ),
        out_shape=(
            jax.ShapeDtypeStruct((TILES * ROWS, TN), jnp.float32),
            jax.ShapeDtypeStruct((ROWS, D), jnp.bfloat16),
            jax.ShapeDtypeStruct((2, 32, LANES), jnp.float32),
        ),
        compiler_params=pltpu.CompilerParams(vmem_limit_bytes=VMEM_LIMIT, dimension_semantics=("arbitrary",)),
        cost_estimate=cost(ROWS * D * TN * TILES, 130_000_000),
        name="logits",
    )(ids, y_all, w_t)


def stats_kernel(st, lab_ref, mask_ref, lse_b, wt_b, lab_b, wt_out, lse_out, buf_y, buf_z, buf_c, tmp, ssem, rsem):
    x, c, z, y = axes()
    peers_y = [dev(x, c, z, up(y, n)) for n in STEPS]
    peers_z = [dev(x, c, up(z, n), y) for n in STEPS]
    d_sib = dev(x, 1 - c, z, y)
    barrier = pltpu.get_barrier_semaphore()
    for d in peers_y + peers_z + [d_sib]:
        pl.semaphore_signal(barrier, inc=1, device_id=d, device_id_type=MESH)
    pl.semaphore_wait(barrier, 7)

    def exchange(src, buf, slot, peers, base):
        cps = []
        for n, d in enumerate(peers):
            cp = pltpu.make_async_remote_copy(src_ref=src, dst_ref=buf.at[slot], send_sem=ssem.at[base + n], recv_sem=rsem.at[base + n], device_id=d, device_id_type=MESH)
            cp.start()
            cps.append(cp)
        buf[slot] = src[...]
        return cps

    def combine(buf, n):
        m = buf[0, 0]
        for i in range(1, n):
            m = jnp.maximum(m, buf[i, 0])
        s = buf[0, 1] * jnp.exp(buf[0, 0] - m)
        for i in range(1, n):
            s = s + buf[i, 1] * jnp.exp(buf[i, 0] - m)
        return m, s

    cps = exchange(st, buf_y, y, peers_y, 0)
    lab = lab_ref[...]
    mask = mask_ref[...].astype(jnp.float32)
    wt = mask / jnp.sum(mask)
    wt_out[...] = wt

    def spread(ref, val):
        for i in range(32):
            ref[pl.ds(i * LANES, LANES), :] = jnp.broadcast_to(val[i:i + 1, :], (LANES, LANES)).T

    spread(wt_b, wt)
    spread(lab_b, lab)
    for cp in cps:
        cp.wait()
    m, s = combine(buf_y, 4)
    tmp[0, 0], tmp[0, 1] = m, s
    for cp in exchange(tmp.at[0], buf_z, z, peers_z, 3):
        cp.wait()
    m, s = combine(buf_z, 4)
    tmp[1, 0], tmp[1, 1] = m, s
    for cp in exchange(tmp.at[1], buf_c, c, [d_sib], 6):
        cp.wait()
    m, s = combine(buf_c, 2)
    lse = m + jnp.log(s)
    lse_out[...] = lse
    spread(lse_b, lse)


def stats(st, lm):
    vm = pl.BlockSpec(memory_space=pltpu.VMEM)
    big = jax.ShapeDtypeStruct((ROWS, LANES), jnp.float32)
    small = jax.ShapeDtypeStruct((32, LANES), jnp.float32)
    return pl.pallas_call(
        stats_kernel,
        out_shape=(big, big, jax.ShapeDtypeStruct((ROWS, LANES), jnp.int32), small, small),
        in_specs=[vm] * 3,
        out_specs=(vm,) * 5,
        scratch_shapes=[
            pltpu.VMEM((4, 2, 32, LANES), jnp.float32),
            pltpu.VMEM((4, 2, 32, LANES), jnp.float32),
            pltpu.VMEM((2, 2, 32, LANES), jnp.float32),
            pltpu.VMEM((2, 2, 32, LANES), jnp.float32),
            pltpu.SemaphoreType.DMA((7,)),
            pltpu.SemaphoreType.DMA((7,)),
        ],
        compiler_params=pltpu.CompilerParams(collective_id=1, has_side_effects=True),
        name="stats",
    )(st, lm[:, :, 0].reshape(32, LANES), lm[:, :, 1].reshape(32, LANES))


def dlogits(z, lse, wt, lab, cols, hits=False):
    out, terms = [], []
    for h in HALVES:
        zh = z[:, h * LANES:(h + 1) * LANES]
        p = jnp.exp(zh - lse)
        hit = lab == cols[:, h * LANES:(h + 1) * LANES]
        out.append((wt * (p - jnp.where(hit, 1.0, 0.0))).astype(jnp.bfloat16))
        if hits:
            terms.append(jnp.where(hit, zh * wt, 0.0))
    g = jnp.concatenate(out, axis=1)
    return (g, terms[0] + terms[1]) if hits else g


def columns(ids, tile, left):
    lane = lax.broadcasted_iota(jnp.int32, (1, TN), 1)
    return jnp.where(lane < left, ids[2] * V_LOC + tile * TN + lane, -1)


def dy_kernel(ids, *refs):
    z_refs = (refs[0:2], refs[2:4])
    w_refs = refs[4:6]
    row_refs = (refs[6:9], refs[9:12])
    outs, tl_ref = refs[12:14], refs[14]
    t = pl.program_id(0)

    @pl.when(t == 0)
    def _():
        for o in outs:
            o[...] = jnp.zeros_like(o)
        tl_ref[...] = jnp.zeros_like(tl_ref)

    cols, ws = [], []
    for h in HALVES:
        tile = ids[0] * TILES + 2 * t + h
        left = jnp.where(2 * t + h < TILES, V_LOC - tile * TN, 0)
        cols.append(columns(ids, tile, left))
        keep = lax.broadcasted_iota(jnp.int32, (TN, 1), 0) < left
        ws.append(jnp.where(keep, w_refs[h][...].astype(jnp.float32), 0.0).astype(jnp.bfloat16))
    w = jnp.concatenate(ws, axis=0)
    work = [(p, i) for p in HALVES for i in range(2)]
    gs = []
    tot = jnp.zeros((8, LANES), jnp.float32)
    for k in range(len(work) + 1):
        if k < len(work):
            p, i = work[k]
            rows = pl.ds(i * 256, 256)
            lse, wt, lab = (r[rows, :] for r in row_refs[p])
            parts = []
            for h in HALVES:
                zz = z_refs[h][p][rows, :]
                if h:
                    zz = jnp.where(2 * t + 1 < TILES, zz, -jnp.inf)
                g, term = dlogits(zz, lse, wt, lab, cols[h], True)
                parts.append(g)
                tot = tot + jnp.sum(term.reshape(32, 8, LANES), axis=0)
            gs.append(jnp.concatenate(parts, axis=1))
        if k:
            p, i = work[k - 1]
            outs[p][pl.ds(i * 256, 256), :] += jnp.dot(gs[k - 1], w, preferred_element_type=jnp.float32)
    tl_ref[...] += tot


def half_block(p, s):
    return 2 * s[1] + (s[0] if p else 1 - s[0])


def dy_partial(ids, z, w_t, lse_b, wt_b, lab_b):
    last = TILES - 1
    fixed, half = row_block((OWN, D), lambda t, s: 0), jax.ShapeDtypeStruct((OWN, D), jnp.float32)

    def zs(h, p):
        return row_block((OWN, TN), lambda t, s: jnp.minimum(2 * t + h, last) * 8 + half_block(p, s))

    def rs(p):
        return row_block((OWN, LANES), lambda t, s: half_block(p, s))

    def wsp(h):
        return row_block((TN, D), lambda t, s: s[0] * TILES + jnp.minimum(2 * t + h, last))

    return pl.pallas_call(
        dy_kernel,
        grid_spec=pltpu.PrefetchScalarGridSpec(
            num_scalar_prefetch=1,
            grid=((TILES + 1) // 2,),
            in_specs=[zs(0, 0), zs(0, 1), zs(1, 0), zs(1, 1), wsp(0), wsp(1)] + [rs(0)] * 3 + [rs(1)] * 3,
            out_specs=(fixed, fixed, row_block((8, LANES), lambda t, s: 0)),
        ),
        out_shape=(half, half, jax.ShapeDtypeStruct((8, LANES), jnp.float32)),
        compiler_params=pltpu.CompilerParams(vmem_limit_bytes=VMEM_LIMIT, dimension_semantics=("arbitrary",)),
        cost_estimate=cost(CHIP_ROWS * D * TN * TILES, 45_000_000),
        name="dy_partial",
    )(ids, z, z, z, z, w_t, w_t, lse_b, wt_b, lab_b, lse_b, wt_b, lab_b)


KC = 512


def dw_kernel(j0, n_own, n_recv, recv_j0, has_prev, *refs):
    refs = list(refs)
    ids = refs.pop(0)
    if has_prev:
        refs.pop(0)
    z, y, lse, wt, lab = refs[:5]
    refs = refs[5:]
    recv = refs.pop(0) if n_recv else None
    o, s, yv, g, acc, obuf, ysem, sems, *rest = refs
    mbuf, msems = rest if n_recv else (None, None)
    t = pl.program_id(0)
    per = -(-n_recv // n_own) if n_recv else 0
    slot = lax.rem(t, 2)

    def o_start(step):
        return pl.multiple_of((ids[0] * TILES + j0 + step) * TN, TN)

    def s_copy(step, sl):
        return pltpu.make_async_copy(obuf.at[sl], s.at[pl.ds(pl.multiple_of(step * TN, TN), TN)], sems.at[sl])

    def o_copy(step, sl, rows):
        return pltpu.make_async_copy(obuf.at[sl, pl.ds(0, rows)], o.at[pl.ds(o_start(step), rows)], sems.at[2 + sl])

    edge = V_LOC % TN
    has_edge = j0 + n_own == TILES
    cut = (ids[0] == 1) if has_edge else None

    def m_in(step, k):
        return pltpu.make_async_copy(recv.at[pl.ds(pl.multiple_of((step * per + k) * TN, TN), TN)], mbuf.at[k], msems.at[k])

    def m_out(step, k):
        row = ((1 - ids[0]) * TILES + recv_j0 + step * per + k) * TN
        return pltpu.make_async_copy(mbuf.at[k], o.at[pl.ds(pl.multiple_of(row, TN), TN)], msems.at[per + k])

    def each_m(step, f):
        for k in range(per):
            @pl.when(step * per + k < n_recv)
            def _(k=k):
                f(step, k)

    n = ROWS // KC

    @pl.when(t == 0)
    def _():
        cp = pltpu.make_async_copy(y, yv, ysem)
        cp.start()
        cp.wait()

    @pl.when(t >= 2)
    def _():
        s_copy(t - 2, slot).wait()
        o_copy(t - 2, slot, TN).wait()

    if n_recv:
        @pl.when(t >= 1)
        def _():
            each_m(t - 1, lambda st, k: m_out(st, k).wait())
        each_m(t, lambda st, k: m_in(st, k).start())

    tile = ids[0] * TILES + j0 + t
    cols = columns(ids, tile, V_LOC - tile * TN)

    for i in range(n + 1):
        if i < n:
            rows = pl.ds(i * KC, KC)
            g[rows, :] = dlogits(z[rows, :], lse[rows, :], wt[rows, :], lab[rows, :], cols)
        if i:
            rows = pl.ds((i - 1) * KC, KC)
            d = lax.dot_general(g[rows, :], yv[rows, :], (((0,), (0,)), ((), ())), preferred_element_type=jnp.float32)
            if i == 1:
                acc[...] = d
            elif i < n:
                acc[...] += d
            else:
                obuf[slot] = acc[...] + d

    s_copy(t, slot).start()
    if has_edge:
        short = cut & (t == n_own - 1)

        @pl.when(short)
        def _():
            o_copy(t, slot, edge).start()

        @pl.when(jnp.logical_not(short))
        def _():
            o_copy(t, slot, TN).start()
    else:
        o_copy(t, slot, TN).start()
    if n_recv:
        def turn(st, k):
            m_in(st, k).wait()
            m_out(st, k).start()
        each_m(t, turn)

    @pl.when(t == n_own - 1)
    def _():
        s_copy(t - 1, 1 - slot).wait()
        o_copy(t - 1, 1 - slot, TN).wait()
        s_copy(t, slot).wait()
        if has_edge:
            @pl.when(cut)
            def _():
                o_copy(t, slot, edge).wait()

            @pl.when(jnp.logical_not(cut))
            def _():
                o_copy(t, slot, TN).wait()
        else:
            o_copy(t, slot, TN).wait()
        if n_recv:
            each_m(t, lambda st, k: m_out(st, k).wait())


def dw_call(ids, o_prev, own, j0, n_own, recv=None, recv_j0=0):
    n_recv = recv.shape[0] // TN if recv is not None else 0
    per = -(-n_recv // n_own) if n_recv else 0
    any_spec = pl.BlockSpec(memory_space=pl.ANY)
    whole = pl.BlockSpec((ROWS, LANES), lambda t, s: (0, 0), pipeline_mode=pl.Buffered(1))
    args, specs, aliases = [], [], {}
    if o_prev is not None:
        aliases = {1: 0}
        args.append(o_prev)
        specs.append(any_spec)
    args += list(own)
    specs += [row_block((ROWS, TN), lambda t, s: j0 + t), any_spec, whole, whole, whole]
    scratch = [
        pltpu.VMEM((ROWS, D), jnp.bfloat16),
        pltpu.VMEM((ROWS, TN), jnp.bfloat16),
        pltpu.VMEM((TN, D), jnp.float32),
        pltpu.VMEM((2, TN, D), jnp.float32),
        pltpu.SemaphoreType.DMA,
        pltpu.SemaphoreType.DMA((4,)),
    ]
    if n_recv:
        args.append(recv)
        specs.append(any_spec)
        scratch += [pltpu.VMEM((per, TN, D), jnp.float32), pltpu.SemaphoreType.DMA((2 * per,))]
    return pl.pallas_call(
        functools.partial(dw_kernel, j0, n_own, n_recv, recv_j0, o_prev is not None),
        grid_spec=pltpu.PrefetchScalarGridSpec(num_scalar_prefetch=1, grid=(n_own,), in_specs=specs, out_specs=(any_spec, any_spec), scratch_shapes=scratch),
        out_shape=(jax.ShapeDtypeStruct((V_LOC, D), jnp.float32), jax.ShapeDtypeStruct((n_own * TN, D), jnp.float32)),
        input_output_aliases=aliases,
        compiler_params=pltpu.CompilerParams(vmem_limit_bytes=VMEM_LIMIT, dimension_semantics=("arbitrary",)),
        cost_estimate=cost(ROWS * D * TN * n_own, (ROWS * TN * 4 + D * TN * 8) * n_own + D * TN * 8 * n_recv),
        name="dw",
    )(ids, *args)


def put_kernel(j0, n, ids, o_prev, recv, o, buf, sems):
    edge = V_LOC % TN
    has_edge = j0 + n == TILES
    cut = ids[0] == 0

    def take(k):
        return pltpu.make_async_copy(recv.at[pl.ds(k * TN, TN)], buf.at[k], sems.at[k])

    def put(k, rows):
        row = pl.multiple_of(((1 - ids[0]) * TILES + j0 + k) * TN, TN)
        return pltpu.make_async_copy(buf.at[k, pl.ds(0, rows)], o.at[pl.ds(row, rows)], sems.at[n + k])

    def each(k, f):
        if has_edge and k == n - 1:
            @pl.when(cut)
            def _():
                f(put(k, edge))

            @pl.when(jnp.logical_not(cut))
            def _():
                f(put(k, TN))
        else:
            f(put(k, TN))

    for k in range(n):
        take(k).start()
    for k in range(n):
        take(k).wait()
        each(k, lambda cp: cp.start())
    for k in range(n):
        each(k, lambda cp: cp.wait())


def put_call(ids, o_prev, recv, j0):
    n = recv.shape[0] // TN
    any_spec = pl.BlockSpec(memory_space=pl.ANY)
    return pl.pallas_call(
        functools.partial(put_kernel, j0, n),
        grid_spec=pltpu.PrefetchScalarGridSpec(
            num_scalar_prefetch=1,
            grid=(1,),
            in_specs=[any_spec, any_spec],
            out_specs=any_spec,
            scratch_shapes=[pltpu.VMEM((n, TN, D), jnp.float32), pltpu.SemaphoreType.DMA((2 * n,))],
        ),
        out_shape=jax.ShapeDtypeStruct((V_LOC, D), jnp.float32),
        input_output_aliases={1: 0},
        compiler_params=pltpu.CompilerParams(vmem_limit_bytes=40_000_000, dimension_semantics=("arbitrary",)),
        cost_estimate=cost(TN, TN * D * 8 * n),
        name="put",
    )(ids, o_prev, recv)


def sum_kernel(tot, out, v, buf_x, buf_c, tmp, ssem, rsem, lsem):
    x, c, z, y = axes()
    cp = pltpu.make_async_copy(tot.at[pl.ds(OWN, 8)], v, lsem.at[0])
    cp.start()
    peers = [dev(up(x, n), c, z, y) for n in STEPS]
    d_sib = dev(x, 1 - c, z, y)
    barrier = pltpu.get_barrier_semaphore()
    for d in (*peers, d_sib):
        pl.semaphore_signal(barrier, inc=1, device_id=d, device_id_type=MESH)
    pl.semaphore_wait(barrier, 4)
    cp.wait()

    def remote(src, dst, k, d):
        return pltpu.make_async_remote_copy(src_ref=src, dst_ref=dst, send_sem=ssem.at[k], recv_sem=rsem.at[k], device_id=d, device_id_type=MESH)

    cps = [remote(v, buf_x.at[x], n, d) for n, d in enumerate(peers)]
    for cp in cps:
        cp.start()
    buf_x[x] = v[...]
    for cp in cps:
        cp.wait()
    tmp[...] = (buf_x[0] + buf_x[1]) + (buf_x[2] + buf_x[3])
    cp = remote(tmp, buf_c.at[c], 3, d_sib)
    cp.start()
    buf_c[c] = tmp[...]
    cp.wait()
    out[...] = buf_c[0] + buf_c[1]


def sum_dp(tot):
    def buf(*n):
        return pltpu.VMEM((*n, 8, D), jnp.float32)

    sems = pltpu.SemaphoreType.DMA((4,))
    return pl.pallas_call(
        sum_kernel,
        out_shape=jax.ShapeDtypeStruct((8, D), jnp.float32),
        in_specs=[pl.BlockSpec(memory_space=pl.ANY)],
        out_specs=pl.BlockSpec(memory_space=pltpu.VMEM),
        scratch_shapes=[buf(), buf(4), buf(2), buf(), sems, sems, pltpu.SemaphoreType.DMA((1,))],
        compiler_params=pltpu.CompilerParams(collective_id=2, has_side_effects=True),
        name="sum_dp",
    )(tot)


def solution(mesh):
    swap = [(i, i ^ 1) for i in range(8)]

    def local_head(hidden, labels, loss_mask, norm_gain, w_out):
        tp, dp = lax.axis_index("tp"), lax.axis_index("dp")
        x, c = dp // 2, dp % 2
        ids = jnp.stack([c, x, tp]).astype(jnp.int32)
        gain_f = norm_gain.astype(jnp.float32)
        h_f32 = hidden.astype(jnp.float32)
        r_inv = lax.rsqrt(jnp.mean(h_f32 * h_f32, axis=-1, keepdims=True) + NORM_EPS)
        x_hat = h_f32 * r_inv
        yf = x_hat * gain_f
        lm = jnp.stack([labels.reshape(4, LANES), loss_mask.reshape(4, LANES)])
        y_all, lm_all = gather(yf, lm)
        w_t = w_out.T
        z, y_bf, st = logits(ids, y_all, w_t)
        lse_b, wt_b, lab_b, wt, lse = stats(st, lm_all)
        other, mine, tl = dy_partial(ids, z, w_t, lse_b, wt_b, lab_b)

        got = lax.ppermute(other, "dp", swap)
        z, tl = lax.optimization_barrier((z, tl))
        own_args = (z, y_bf, lse_b, wt_b, lab_b)
        o, s0 = dw_call(ids, None, own_args, 0, CHUNKS[0])
        recv0 = lax.ppermute(s0, "dp", swap)
        dy_c = mine + got
        dgain_p = jnp.sum(dy_c * x_hat, axis=0)
        wl = (wt * lse).reshape(8, 4, LANES)
        own_wl = jnp.where(tp == 0, jnp.sum(lax.dynamic_index_in_dim(wl, dp, 0, keepdims=False)), 0.0)
        loss_p = own_wl - jnp.sum(tl)
        extra = jnp.zeros((8, D), jnp.float32).at[0].set(dgain_p).at[1, 0].set(loss_p)
        part = jnp.concatenate([dy_c, extra], axis=0)
        part, o = lax.optimization_barrier((part, o))
        tot = lax.psum(part, "tp")
        o, s1 = dw_call(ids, o, own_args, CHUNKS[0], CHUNKS[1])
        recv1 = lax.ppermute(s1, "dp", swap)
        o, s2 = dw_call(ids, o, own_args, CHUNKS[0] + CHUNKS[1], CHUNKS[2], recv0, 0)
        recv2 = lax.ppermute(s2, "dp", swap)
        o = put_call(ids, o, recv1, CHUNKS[0])
        d_normed = tot[:OWN]
        small = sum_dp(tot)
        u = d_normed * gain_f
        d_hidden = r_inv * (u - x_hat * jnp.mean(u * x_hat, axis=-1, keepdims=True))
        d_hidden = d_hidden.astype(jnp.bfloat16)
        o, small, d_hidden = lax.optimization_barrier((o, small, d_hidden))
        o = put_call(ids, o, recv2, CHUNKS[0] + CHUNKS[1])
        loss_total, d_gain = small[1, 0], small[0]
        return loss_total, d_hidden, o.T, d_gain

    return jax.shard_map(local_head, mesh=mesh, in_specs=(P("dp", None), P("dp"), P("dp"), P(), P(None, "tp")), out_specs=(P(), P("dp", None), P(None, "tp"), P()), check_vma=False)
```
